32 devices in a mesh: ta: 2 (over x), gz: 4 (over z), xy: 4 (over y, core).
Axes of the slice: x: 2, y: 2, z: 4, core: 2. Of those that a mesh axis runs over, the one named last changes fastest.
Arguments:
- source: float32 [2, 48, 2, 4, 512], P(None, None, 'ta', 'gz', 'xy'), may hold values from -14 to 14
- inverse: bfloat16 [2, 48, 48, 2, 4, 512], P(None, None, None, 'ta', 'gz', 'xy'), may hold values from -0.625 to 0.625
- coarse_links: bfloat16 [8, 2, 48, 48, 2, 4, 512], P(None, None, None, None, 'ta', 'gz', 'xy'), may hold values from -0.15625 to 0.15625
Outputs:
- solution: float32 [2, 48, 2, 4, 512], P(None, None, 'ta', 'gz', 'xy')
- residual: float32 [2, 48, 2, 4, 512], P(None, None, 'ta', 'gz', 'xy')
- hessenberg: float32 [2, 6, 5], replicated
The draws below stay inside these ranges and needn't reach their ends.
All inputs are finite; a program needn't handle non-finite values.
Results may differ from the reference program's by a relative error of at most 0.0003.
Values sent between devices are 32-bit elements; how exact they have to be, the bound alone decides.
A program may use at most 128 MiB of HBM per device.

```python
import jax
import jax.numpy as jnp
from jax import lax

COMP = 48
LY = 16
ITERS = 5
NT = 2
NZ = 4
NXY = 512


def draw_source(key, part):
    key_scale, key_noise = jax.random.split(jax.random.fold_in(key, 11))
    time_pos = jnp.arange(NT).astype(jnp.float32)[:, None, None] / max(NT - 1, 1)
    spread = jax.random.uniform(key_scale, (NT, NZ, NXY), jnp.float32)
    site_scale = 10.0 ** (0.5 * time_pos + 0.5 * spread) / 3.0
    fluctuation = jnp.clip(jax.random.normal(key_noise, (2, COMP, NT, NZ, NXY), jnp.float32), -4.0, 4.0)
    values = fluctuation * site_scale
    return values


def block_levels(own_key, extent, cuts, smallest, top_value):
    loudness = 1.0
    for dim, blocks in cuts:
        draws = jax.random.uniform(jax.random.fold_in(jax.random.fold_in(own_key, 6), dim), (blocks,), jnp.float32, smallest / len(cuts), top_value / len(cuts))
        loudness = loudness * jnp.repeat(jnp.exp(draws), extent[dim] // blocks).reshape((-1,) + (1,) * (len(extent) - 1 - dim))
    return loudness


def scatter_about(rng, shape, width, most, shards=(), dtype=jnp.bfloat16):
    array = jax.random.normal(rng, shape, jnp.float32) * width
    if len(shards) > 0:
        array = block_levels(rng, shape, shards, -0.22, 0.18) * array
    return jnp.clip(array, min=-most, max=most).astype(dtype)


def setup_inputs(seed: int = 0) -> dict:
    key_of = jax.random.split(jax.random.key(seed), 4)
    source = draw_source(jax.random.fold_in(key_of[3], 71), 0)
    inverse = scatter_about(key_of[1], (2, COMP, COMP, NT, NZ, NXY), (2 * COMP) ** -0.5, 0.625, ((3, 2), (4, 4), (5, 4)))
    coarse_links = scatter_about(key_of[2], (8, 2, COMP, COMP, NT, NZ, NXY), (32 * COMP) ** -0.5, 0.15625, ((4, 2), (5, 4), (6, 4)))
    return dict(source=source, inverse=inverse, coarse_links=coarse_links)


def contract(matrix, part):
    return jnp.einsum('ijtzs,jtzs->itzs', matrix, part, precision=lax.Precision.HIGHEST)

def block_apply(blocks, vector):
    widened = blocks.astype(jnp.float32)
    real_part = contract(widened[0], vector[0]) - contract(widened[1], vector[1])
    imag_part = contract(widened[0], vector[1]) + contract(widened[1], vector[0])
    return jnp.stack([real_part, imag_part])

def complex_dot(left, right):
    real_part = jnp.sum(left[0] * right[0] + left[1] * right[1])
    imag_part = jnp.sum(left[0] * right[1] - left[1] * right[0])
    return (real_part, imag_part)

def scaled(coef_real, coef_imag, vector):
    return jnp.stack([coef_real * vector[0] - coef_imag * vector[1], coef_real * vector[1] + coef_imag * vector[0]])

def y_neighbours(field):
    positions = jnp.arange(field.shape[4]) % LY
    is_last = positions == LY - 1
    is_first = positions == 0
    forward = jnp.where(is_last, jnp.roll(field, LY - 1, axis=4), jnp.roll(field, -1, axis=4))
    backward = jnp.where(is_first, jnp.roll(field, 1 - LY, axis=4), jnp.roll(field, 1, axis=4))
    return (forward, backward)

def neighbour_fields(field):
    forward_y, backward_y = y_neighbours(field)
    return [jnp.roll(field, -1, axis=2), jnp.roll(field, 1, axis=2), jnp.roll(field, -1, axis=3), jnp.roll(field, 1, axis=3), jnp.roll(field, -LY, axis=4), jnp.roll(field, LY, axis=4), forward_y, backward_y]

def apply_operator(field, inverse, coarse_links):
    neighbours = neighbour_fields(field)
    hopping = block_apply(coarse_links[0], neighbours[0])
    for d in range(1, 8):
        hopping = hopping + block_apply(coarse_links[d], neighbours[d])
    return field + block_apply(inverse, hopping)

def solve_small(hessenberg, source_norm):
    upper_half = jnp.concatenate([hessenberg[0], -hessenberg[1]], axis=1)
    lower_half = jnp.concatenate([hessenberg[1], hessenberg[0]], axis=1)
    real_form = jnp.concatenate([upper_half, lower_half], axis=0)
    target = jnp.zeros((2 * (ITERS + 1),), jnp.float32).at[0].set(source_norm)
    normal_mat = jnp.dot(real_form.T, real_form, precision=lax.Precision.HIGHEST)
    projected = jnp.dot(real_form.T, target, precision=lax.Precision.HIGHEST)
    factor = jnp.linalg.cholesky(normal_mat)
    forward_vals = []
    for i in range(2 * ITERS):
        partial_sum = projected[i]
        for k in range(i):
            partial_sum = partial_sum - factor[i, k] * forward_vals[k]
        forward_vals.append(partial_sum / factor[i, i])
    solved = [None] * (2 * ITERS)
    for i in reversed(range(2 * ITERS)):
        partial_sum = forward_vals[i]
        for k in range(i + 1, 2 * ITERS):
            partial_sum = partial_sum - factor[k, i] * solved[k]
        solved[i] = partial_sum / factor[i, i]
    coeffs = jnp.stack(solved)
    return (coeffs[:ITERS], coeffs[ITERS:], target)

def reference(source, inverse, coarse_links):
    norm_sq = complex_dot(source, source)[0]
    source_norm = jnp.sqrt(norm_sq)
    krylov_basis = [source / source_norm]
    hessenberg = jnp.zeros((2, ITERS + 1, ITERS), jnp.float32)
    for j in range(ITERS):
        candidate = apply_operator(krylov_basis[j], inverse, coarse_links)
        products = [complex_dot(krylov_basis[i], candidate) for i in range(j + 1)]
        for i in range(j + 1):
            candidate = candidate - scaled(products[i][0], products[i][1], krylov_basis[i])
            hessenberg = hessenberg.at[0, i, j].set(products[i][0]).at[1, i, j].set(products[i][1])
        length = jnp.sqrt(complex_dot(candidate, candidate)[0])
        hessenberg = hessenberg.at[0, j + 1, j].set(length)
        krylov_basis.append(candidate / length)
    coef_real, coef_imag, target = solve_small(hessenberg, source_norm)
    solution = scaled(coef_real[0], coef_imag[0], krylov_basis[0])
    for j in range(1, ITERS):
        solution = solution + scaled(coef_real[j], coef_imag[j], krylov_basis[j])
    residual = source - apply_operator(solution, inverse, coarse_links)
    return (solution, residual, hessenberg)
```

```python
import functools

import jax
import jax.numpy as jnp
from jax import lax
from jax.experimental import pallas as pl
from jax.experimental.pallas import tpu as pltpu
from jax.sharding import PartitionSpec as P

LY = 16
ITERS = 5
SUB = 8
MESH = pl.DeviceIdType.MESH
ARRIVAL = (6, 7, 4, 5, 0, 1, 2, 3)


def cmul(a, b):
    return (a[0] * b[0] - a[1] * b[1], a[0] * b[1] + a[1] * b[0])


def cmul_conj(a, b):
    return (a[0] * b[0] + a[1] * b[1], a[0] * b[1] - a[1] * b[0])


def csub(a, b):
    return (a[0] - b[0], a[1] - b[1])


def cscale(a, s):
    return (a[0] * s, a[1] * s)


def kernel(sizes, source_hbm, inverse_hbm, links_hbm, sol_ref, res_ref, hes_ref,
           stage, mat_a, mat_b, mat_s, vecs, acc, src, fields, vs, qs,
           halo_t, halo_z, halo_x, pack, red_one, red_two, row_one, row_two,
           load_sem, src_sem, t_send, t_recv, z_send, z_recv, x_send, x_recv,
           one_send, one_recv, two_send, two_recv):
    n_ta, n_gz, n_xy = sizes
    comp, lanes = src.shape[1], src.shape[2]
    tiles = comp // SUB
    me_ta, me_gz, me_xy = (lax.axis_index(a) for a in ("ta", "gz", "xy"))
    n_two = n_ta * n_gz
    me_two = me_ta * n_gz + me_gz

    pltpu.make_async_copy(source_hbm, src, src_sem).start()
    loads = []
    for d in ARRIVAL:
        loads.append(pltpu.make_async_copy(links_hbm.at[d], stage.at[d], load_sem.at[d]))
    loads.append(pltpu.make_async_copy(inverse_hbm, stage.at[8], load_sem.at[8]))
    for load in loads:
        load.start()

    def two_peer(k):
        p = lax.rem(me_two + k, n_two)
        return p, {"ta": p // n_gz, "gz": lax.rem(p, n_gz)}

    barrier = pltpu.get_barrier_semaphore()
    for k in range(1, n_xy):
        pl.semaphore_signal(barrier, inc=1, device_id={"xy": lax.rem(me_xy + k, n_xy)}, device_id_type=MESH)
    for k in range(1, n_two):
        pl.semaphore_signal(barrier, inc=1, device_id=two_peer(k)[1], device_id_type=MESH)
    pltpu.make_async_copy(source_hbm, src, src_sem).wait()
    pl.semaphore_wait(barrier, n_xy - 1 + n_two - 1)

    lane = lax.broadcasted_iota(jnp.int32, (SUB, lanes), 1)
    lane_all = lax.broadcasted_iota(jnp.int32, (comp, lanes), 1)
    pending = []

    def remote(s, d, send, recv, device):
        return pltpu.make_async_remote_copy(
            src_ref=s, dst_ref=d, send_sem=send, recv_sem=recv, device_id=device, device_id_type=MESH)

    def packed(value, first):
        out = jnp.zeros((SUB, lanes), jnp.float32)
        for k in range(tiles):
            tile = value[k * SUB:(k + 1) * SUB]
            shift = (LY * k + (0 if first else LY)) % lanes
            if shift:
                tile = pltpu.roll(tile, shift, 1)
            out = jnp.where(lane // LY == k, tile, out)
        return out

    def unpacked(value, first):
        out = []
        for k in range(tiles):
            shift = ((0 if first else lanes - LY) - LY * k) % lanes
            out.append(pltpu.roll(value, shift, 1) if shift else value)
        return jnp.concatenate(out, axis=0)

    def send_halo(e, ref):
        for c in range(2):
            value = ref[c]
            pack[e, 0, c] = packed(value, True)
            pack[e, 1, c] = packed(value, False)
        waits = {}
        for slot, step in ((0, n_xy - 1), (1, 1)):
            cp = remote(pack.at[e, slot], halo_x.at[e, slot], x_send.at[e, slot], x_recv.at[e, slot],
                        {"xy": lax.rem(me_xy + step, n_xy)})
            cp.start()
            pending.append(cp)
            waits["x", slot] = cp
        for slot, step in ((0, n_gz - 1), (1, 1)):
            cp = remote(ref, halo_z.at[e, slot], z_send.at[e, slot], z_recv.at[e, slot],
                        {"gz": lax.rem(me_gz + step, n_gz)})
            cp.start()
            pending.append(cp)
            waits["z", slot] = cp
        for slot, step in ((0, n_ta - 1), (1, 1))[:1 if n_ta == 2 else 2]:
            cp = remote(ref, halo_t.at[e, slot], t_send.at[e, slot], t_recv.at[e, slot],
                        {"ta": lax.rem(me_ta + step, n_ta)})
            cp.start()
            pending.append(cp)
            waits["t", slot] = cp
        return waits

    def put(slot, re, im):
        vecs[slot, 0] = re
        vecs[slot, 1] = im - re
        vecs[slot, 2] = re + im

    def set_y(ref):
        pos = lane_all % LY
        fwd, bwd = [], []
        for c in range(2):
            v = ref[c]
            fwd.append(jnp.where(pos == LY - 1, pltpu.roll(v, LY - 1, 1), pltpu.roll(v, lanes - 1, 1)))
            bwd.append(jnp.where(pos == 0, pltpu.roll(v, lanes - LY + 1, 1), pltpu.roll(v, 1, 1)))
        put(6, *fwd)
        put(7, *bwd)

    def set_x(e, ref, waits):
        fwd, bwd = [], []
        waits["x", 0].wait_recv()
        waits["x", 1].wait_recv()
        for c in range(2):
            v = ref[c]
            fwd.append(jnp.where(lane_all >= lanes - LY, unpacked(halo_x[e, 0, c], False), pltpu.roll(v, lanes - LY, 1)))
            bwd.append(jnp.where(lane_all < LY, unpacked(halo_x[e, 1, c], True), pltpu.roll(v, LY, 1)))
        put(4, *fwd)
        put(5, *bwd)

    def set_t(e, waits):
        waits["t", 0].wait_recv()
        put(0, halo_t[e, 0, 0], halo_t[e, 0, 1])
        back = 0
        if n_ta != 2:
            waits["t", 1].wait_recv()
            back = 1
        put(1, halo_t[e, back, 0], halo_t[e, back, 1])

    def set_z(e, waits):
        for slot in range(2):
            waits["z", slot].wait_recv()
            put(2 + slot, halo_z[e, slot, 0], halo_z[e, slot, 1])

    def convert(d):
        def body(i, _):
            rows = pl.ds(i * 2, 2)
            a = stage[d, 0, rows].astype(jnp.float32)
            b = stage[d, 1, rows].astype(jnp.float32)
            mat_a[d, rows] = a
            mat_b[d, rows] = b
            mat_s[d, rows] = a + b
            return 0

        lax.fori_loop(0, comp // 2, body, 0)

    def products(dirs, first, out=None):
        def body(b, _):
            rows = pl.ds(b * SUB, SUB)
            if first:
                sums = [jnp.zeros((SUB, SUB, lanes), jnp.float32)] * 3
            else:
                sums = [acc[m, rows] for m in range(3)]
            for d in dirs:
                slot = 0 if d == 8 else d
                for k in range(tiles):
                    cols = pl.ds(k * SUB, SUB)
                    for m, mat in enumerate((mat_s, mat_a, mat_b)):
                        sums[m] = sums[m] + mat[d, rows, cols] * vecs[slot, m, cols][None]
            if out is None:
                for m in range(3):
                    acc[m, rows] = sums[m]
            else:
                out[0, rows] = jnp.sum(sums[0] - sums[2], axis=1)
                out[1, rows] = jnp.sum(sums[0] + sums[1], axis=1)
            return 0

        lax.fori_loop(0, comp // SUB, body, 0)

    def finish_apply(out):
        put(0, fields[0, 0], fields[0, 1])
        products((8,), True, out)

    row16 = lax.broadcasted_iota(jnp.int32, (2 * SUB, lanes), 0)
    lane16 = lax.broadcasted_iota(jnp.int32, (2 * SUB, lanes), 1)

    def start_reduce(j, values):
        table = jnp.zeros((2 * SUB, lanes), jnp.float32)
        for k, value in enumerate(values):
            table = jnp.where(row16 == k, jnp.sum(value, axis=0, keepdims=True), table)
        table = jnp.sum(table, axis=1, keepdims=True)
        row = jnp.sum(jnp.where(row16 == lane16, table, 0.0), axis=0, keepdims=True)
        row_one[j] = row
        for k in range(1, n_xy):
            cp = remote(row_one.at[j], red_one.at[j, me_xy], one_send.at[j, k], one_recv.at[j, me_xy],
                        {"xy": lax.rem(me_xy + k, n_xy)})
            cp.start()
            pending.append(cp)
        red_one[j, me_xy] = row

    def middle_reduce(j):
        for k in range(1, n_xy):
            p = lax.rem(me_xy + n_xy - k, n_xy)
            remote(row_one.at[j], red_one.at[j, p], one_send.at[j, k], one_recv.at[j, p], {"xy": p}).wait_recv()
        row = red_one[j, 0]
        for k in range(1, n_xy):
            row = row + red_one[j, k]
        row_two[j] = row
        for k in range(1, n_two):
            cp = remote(row_two.at[j], red_two.at[j, me_two], two_send.at[j, k], two_recv.at[j, me_two], two_peer(k)[1])
            cp.start()
            pending.append(cp)
        red_two[j, me_two] = row

    def end_reduce(j, count):
        for k in range(1, n_two):
            p, device = two_peer(n_two - k)
            remote(row_two.at[j], red_two.at[j, p], two_send.at[j, k], two_recv.at[j, p], device).wait_recv()
        row = red_two[j, 0]
        for k in range(1, n_two):
            row = row + red_two[j, k]
        return [jnp.broadcast_to(row[:, k:k + 1], (1, lanes)) for k in range(count)]

    def load(ref):
        return (ref[0], ref[1])

    def store(ref, value):
        ref[0] = value[0]
        ref[1] = value[1]

    def dots(vector_refs, q):
        values = []
        for ref in vector_refs:
            values.extend(cmul_conj(load(ref), q))
        values.append(q[0] * q[0] + q[1] * q[1])
        return values

    waits = send_halo(0, src)
    for at, d in enumerate(ARRIVAL):
        if d == 6:
            set_y(src)
        elif d == 4:
            set_x(0, src, waits)
        elif d == 0:
            set_t(0, waits)
        elif d == 2:
            set_z(0, waits)
        loads[at].wait()
        convert(d)
        products((d,), at == 0, fields.at[0] if at == 7 else None)
    loads[8].wait()
    convert(8)
    raw = fields.at[1]
    finish_apply(raw)

    def apply(e, ref, out, j):
        set_y(ref)
        products((6, 7), True)
        middle_reduce(j)
        set_x(e, ref, waits)
        products((4, 5), False)
        set_t(e, waits)
        set_z(e, waits)
        products((0, 1, 2, 3), False, fields.at[0])
        finish_apply(out)

    waits = send_halo(1, raw)
    source = load(src)
    q = load(raw)
    start_reduce(0, dots([src], q) + [source[0] * source[0] + source[1] * source[1]])
    product = fields.at[2]
    apply(1, raw, product, 0)
    dot_re, dot_im, q_sq, norm_sq = end_reduce(0, 4)
    source_norm = jnp.sqrt(norm_sq)
    scale = 1.0 / source_norm
    store(vs.at[0], cscale(load(src), scale))
    store(qs.at[0], cscale(load(raw), scale))
    store(product, cscale(load(product), scale))
    g = [(dot_re * scale * scale, dot_im * scale * scale)]
    q_sq = q_sq * scale * scale

    columns = []
    low = [[None] * ITERS for _ in range(ITERS)]
    inv_diag, forward = [], []

    def factor_row(j):
        entries = []
        for k in range(j + 1):
            total = cmul_conj(columns[j][0], columns[k][0])
            for m in range(1, k + 2):
                term = cmul_conj(columns[j][m], columns[k][m])
                total = (total[0] + term[0], total[1] + term[1])
            entries.append(total)
        for k in range(j):
            total = entries[k]
            for m in range(k):
                total = csub(total, cmul_conj(low[k][m], low[j][m]))
            low[j][k] = cscale(total, inv_diag[k])
        diag = entries[j][0]
        for m in range(j):
            diag = diag - (low[j][m][0] * low[j][m][0] + low[j][m][1] * low[j][m][1])
        inv_diag.append(1.0 / jnp.sqrt(diag))
        total = (source_norm * columns[j][0][0], -source_norm * columns[j][0][1])
        for m in range(j):
            total = csub(total, cmul(low[j][m], forward[m]))
        forward.append(cscale(total, inv_diag[j]))

    zero = jnp.zeros((1, lanes), jnp.float32)
    for j in range(ITERS):
        length_sq = q_sq
        for re, im in g:
            length_sq = length_sq - (re * re + im * im)
        length = jnp.sqrt(length_sq)
        columns.append(g[:j] + [(g[j][0] + 1.0, g[j][1]), (length, zero)])
        if j < ITERS - 1:
            scale = 1.0 / length
            v = load(qs.at[j])
            q = load(product)
            for i in range(j + 1):
                v = csub(v, cmul(g[i], load(vs.at[i])))
                q = csub(q, cmul(g[i], load(qs.at[i])))
            store(qs.at[j + 1], cscale(q, scale))
            store(vs.at[j + 1], cscale(v, scale))
            last = j + 1 == ITERS - 1
            if not last:
                waits = send_halo(j + 2, qs.at[j + 1])
            start_reduce(j + 1, dots([vs.at[i] for i in range(j + 2)], load(qs.at[j + 1])))
            factor_row(j)
            if last:
                middle_reduce(j + 1)
            else:
                product = fields.at[j + 3]
                apply(j + 2, qs.at[j + 1], product, j + 1)
            got = end_reduce(j + 1, 2 * (j + 2) + 1)
            g = [(got[2 * i], got[2 * i + 1]) for i in range(j + 2)]
            q_sq = got[2 * (j + 2)]
        else:
            factor_row(j)

    coeffs = [None] * ITERS
    for j in reversed(range(ITERS)):
        total = forward[j]
        for m in range(j + 1, ITERS):
            total = csub(total, cmul_conj(low[m][j], coeffs[m]))
        coeffs[j] = cscale(total, inv_diag[j])

    answer = cmul(coeffs[0], load(vs.at[0]))
    left = csub(load(src), cmul(coeffs[0], load(qs.at[0])))
    for j in range(1, ITERS):
        term = cmul(coeffs[j], load(vs.at[j]))
        answer = (answer[0] + term[0], answer[1] + term[1])
        left = csub(left, cmul(coeffs[j], load(qs.at[j])))
    store(sol_ref, answer)
    store(res_ref, csub(left, answer))

    shape = hes_ref.shape[1:]
    row = lax.broadcasted_iota(jnp.int32, shape, 0)
    col = lax.broadcasted_iota(jnp.int32, shape, 1)
    for c in range(2):
        table = jnp.zeros(shape, jnp.float32)
        for j in range(ITERS):
            for i in range(j + 2):
                table = jnp.where((row == i) & (col == j), columns[j][i][c][:, :shape[1]], table)
        hes_ref[c] = table

    for cp in pending:
        cp.wait_send()


def solution(mesh):
    sizes = tuple(mesh.shape[a] for a in ("ta", "gz", "xy"))

    def per_device(source, inverse, coarse_links):
        comp, lanes = source.shape[1], source.shape[4]
        f32 = jnp.float32
        field = (2, comp, lanes)
        mats = (9, comp, comp, lanes)
        n_two = sizes[0] * sizes[1]
        dma = pltpu.SemaphoreType.DMA
        hbm = pl.BlockSpec(memory_space=pl.ANY)
        vmem = pl.BlockSpec(memory_space=pltpu.VMEM)
        sol, res, hes = pl.pallas_call(
            functools.partial(kernel, sizes),
            out_shape=(
                jax.ShapeDtypeStruct(field, f32),
                jax.ShapeDtypeStruct(field, f32),
                jax.ShapeDtypeStruct((2, ITERS + 1, ITERS), f32),
            ),
            in_specs=[hbm, hbm, hbm],
            out_specs=(vmem, vmem, vmem),
            scratch_shapes=[
                pltpu.VMEM((9, 2, comp, comp, lanes), coarse_links.dtype),
                pltpu.VMEM(mats, f32),
                pltpu.VMEM(mats, f32),
                pltpu.VMEM(mats, f32),
                pltpu.VMEM((8, 3, comp, lanes), f32),
                pltpu.VMEM((3, comp, SUB, lanes), f32),
                pltpu.VMEM(field, f32),
                pltpu.VMEM((ITERS + 1, *field), f32),
                pltpu.VMEM((ITERS, *field), f32),
                pltpu.VMEM((ITERS, *field), f32),
                pltpu.VMEM((ITERS, 2, *field), f32),
                pltpu.VMEM((ITERS, 2, *field), f32),
                pltpu.VMEM((ITERS, 2, 2, SUB, lanes), f32),
                pltpu.VMEM((ITERS, 2, 2, SUB, lanes), f32),
                pltpu.VMEM((ITERS, sizes[2], 1, lanes), f32),
                pltpu.VMEM((ITERS, n_two, 1, lanes), f32),
                pltpu.VMEM((ITERS, 1, lanes), f32),
                pltpu.VMEM((ITERS, 1, lanes), f32),
                dma((9,)),
                dma,
                dma((ITERS, 2)), dma((ITERS, 2)),
                dma((ITERS, 2)), dma((ITERS, 2)),
                dma((ITERS, 2)), dma((ITERS, 2)),
                dma((ITERS, sizes[2])), dma((ITERS, sizes[2])),
                dma((ITERS, n_two)), dma((ITERS, n_two)),
            ],
            compiler_params=pltpu.CompilerParams(
                collective_id=0, has_side_effects=True, vmem_limit_bytes=60 * 1024 * 1024),
        )(
            source.reshape(field),
            inverse.reshape(2, comp, comp, lanes),
            coarse_links.reshape(8, 2, comp, comp, lanes),
        )
        return sol.reshape(source.shape), res.reshape(source.shape), hes

    specs = (
        P(None, None, "ta", "gz", "xy"),
        P(None, None, None, "ta", "gz", "xy"),
        P(None, None, None, None, "ta", "gz", "xy"),
    )
    return jax.shard_map(
        per_device,
        mesh=mesh,
        in_specs=specs,
        out_specs=(specs[0], specs[0], P()),
        check_vma=False,
    )
```

```python
import functools

import jax
import jax.numpy as jnp
from jax import lax
from jax.experimental import pallas as pl
from jax.experimental.pallas import tpu as pltpu
from jax.sharding import PartitionSpec as P

LY = 16
ITERS = 5
SUB = 8
MESH = pl.DeviceIdType.MESH
ARRIVAL = (6, 7, 4, 5, 0, 1, 2, 3)


def cmul(a, b):
    return (a[0] * b[0] - a[1] * b[1], a[0] * b[1] + a[1] * b[0])


def cmul_conj(a, b):
    return (a[0] * b[0] + a[1] * b[1], a[0] * b[1] - a[1] * b[0])


def csub(a, b):
    return (a[0] - b[0], a[1] - b[1])


def cscale(a, s):
    return (a[0] * s, a[1] * s)


def kernel(sizes, source_hbm, inverse_hbm, links_hbm, sol_ref, res_ref, hes_ref,
           stage, mat_a, mat_b, mat_s, vecs, acc, src, fields, vs, qs,
           halo_t, halo_z, halo_x, pack, red_one, red_two, row_one, row_two,
           load_sem, src_sem, t_send, t_recv, z_send, z_recv, x_send, x_recv,
           one_send, one_recv, two_send, two_recv):
    n_ta, n_gz, n_xy = sizes
    comp, lanes = src.shape[1], src.shape[2]
    tiles = comp // SUB
    me_ta, me_gz, me_xy = (lax.axis_index(a) for a in ("ta", "gz", "xy"))
    n_two = n_ta * n_gz
    me_two = me_ta * n_gz + me_gz

    pltpu.make_async_copy(source_hbm, src, src_sem).start()
    loads = []
    for d in ARRIVAL:
        loads.append(pltpu.make_async_copy(links_hbm.at[d], stage.at[d], load_sem.at[d]))
    loads.append(pltpu.make_async_copy(inverse_hbm, stage.at[8], load_sem.at[8]))
    for load in loads:
        load.start()

    def two_peer(k):
        p = lax.rem(me_two + k, n_two)
        return p, {"ta": p // n_gz, "gz": lax.rem(p, n_gz)}

    barrier = pltpu.get_barrier_semaphore()
    for k in range(1, n_xy):
        pl.semaphore_signal(barrier, inc=1, device_id={"xy": lax.rem(me_xy + k, n_xy)}, device_id_type=MESH)
    for k in range(1, n_two):
        pl.semaphore_signal(barrier, inc=1, device_id=two_peer(k)[1], device_id_type=MESH)
    pltpu.make_async_copy(source_hbm, src, src_sem).wait()
    pl.semaphore_wait(barrier, n_xy - 1 + n_two - 1)

    lane = lax.broadcasted_iota(jnp.int32, (SUB, lanes), 1)
    lane_all = lax.broadcasted_iota(jnp.int32, (comp, lanes), 1)
    pending = []

    def remote(s, d, send, recv, device):
        return pltpu.make_async_remote_copy(
            src_ref=s, dst_ref=d, send_sem=send, recv_sem=recv, device_id=device, device_id_type=MESH)

    def packed(value, first):
        out = jnp.zeros((SUB, lanes), jnp.float32)
        for k in range(tiles):
            tile = value[k * SUB:(k + 1) * SUB]
            shift = (LY * k + (0 if first else LY)) % lanes
            if shift:
                tile = pltpu.roll(tile, shift, 1)
            out = jnp.where(lane // LY == k, tile, out)
        return out

    def unpacked(value, first):
        out = []
        for k in range(tiles):
            shift = ((0 if first else lanes - LY) - LY * k) % lanes
            out.append(pltpu.roll(value, shift, 1) if shift else value)
        return jnp.concatenate(out, axis=0)

    def send_halo(e, ref):
        for c in range(2):
            value = ref[c]
            pack[e, 0, c] = packed(value, True)
            pack[e, 1, c] = packed(value, False)
        waits = {}
        for slot, step in ((0, n_xy - 1), (1, 1)):
            cp = remote(pack.at[e, slot], halo_x.at[e, slot], x_send.at[e, slot], x_recv.at[e, slot],
                        {"xy": lax.rem(me_xy + step, n_xy)})
            cp.start()
            pending.append(cp)
            waits["x", slot] = cp
        for slot, step in ((0, n_gz - 1), (1, 1)):
            cp = remote(ref, halo_z.at[e, slot], z_send.at[e, slot], z_recv.at[e, slot],
                        {"gz": lax.rem(me_gz + step, n_gz)})
            cp.start()
            pending.append(cp)
            waits["z", slot] = cp
        for slot, step in ((0, n_ta - 1), (1, 1))[:1 if n_ta == 2 else 2]:
            cp = remote(ref, halo_t.at[e, slot], t_send.at[e, slot], t_recv.at[e, slot],
                        {"ta": lax.rem(me_ta + step, n_ta)})
            cp.start()
            pending.append(cp)
            waits["t", slot] = cp
        return waits

    def put(slot, re, im):
        vecs[slot, 0] = re
        vecs[slot, 1] = im - re
        vecs[slot, 2] = re + im

    def set_y(ref):
        pos = lane_all % LY
        fwd, bwd = [], []
        for c in range(2):
            v = ref[c]
            fwd.append(jnp.where(pos == LY - 1, pltpu.roll(v, LY - 1, 1), pltpu.roll(v, lanes - 1, 1)))
            bwd.append(jnp.where(pos == 0, pltpu.roll(v, lanes - LY + 1, 1), pltpu.roll(v, 1, 1)))
        put(6, *fwd)
        put(7, *bwd)

    def set_x(e, ref, waits):
        fwd, bwd = [], []
        waits["x", 0].wait_recv()
        waits["x", 1].wait_recv()
        for c in range(2):
            v = ref[c]
            fwd.append(jnp.where(lane_all >= lanes - LY, unpacked(halo_x[e, 0, c], False), pltpu.roll(v, lanes - LY, 1)))
            bwd.append(jnp.where(lane_all < LY, unpacked(halo_x[e, 1, c], True), pltpu.roll(v, LY, 1)))
        put(4, *fwd)
        put(5, *bwd)

    def set_t(e, waits):
        waits["t", 0].wait_recv()
        put(0, halo_t[e, 0, 0], halo_t[e, 0, 1])
        back = 0
        if n_ta != 2:
            waits["t", 1].wait_recv()
            back = 1
        put(1, halo_t[e, back, 0], halo_t[e, back, 1])

    def set_z(e, waits):
        for slot in range(2):
            waits["z", slot].wait_recv()
            put(2 + slot, halo_z[e, slot, 0], halo_z[e, slot, 1])

    def convert(d):
        def body(i, _):
            rows = pl.ds(i * 2, 2)
            a = stage[d, 0, rows].astype(jnp.float32)
            b = stage[d, 1, rows].astype(jnp.float32)
            mat_a[d, rows] = a
            mat_b[d, rows] = b
            mat_s[d, rows] = a + b
            return 0

        lax.fori_loop(0, comp // 2, body, 0)

    def products(dirs, first, out=None):
        def body(b, _):
            rows = pl.ds(b * SUB, SUB)
            if first:
                sums = [jnp.zeros((SUB, SUB, lanes), jnp.float32)] * 3
            else:
                sums = [acc[m, rows] for m in range(3)]
            for d in dirs:
                slot = 0 if d == 8 else d
                for k in range(tiles):
                    cols = pl.ds(k * SUB, SUB)
                    for m, mat in enumerate((mat_s, mat_a, mat_b)):
                        sums[m] = sums[m] + mat[d, rows, cols] * vecs[slot, m, cols][None]
            if out is None:
                for m in range(3):
                    acc[m, rows] = sums[m]
            else:
                out[0, rows] = jnp.sum(sums[0] - sums[2], axis=1)
                out[1, rows] = jnp.sum(sums[0] + sums[1], axis=1)
            return 0

        lax.fori_loop(0, comp // SUB, body, 0)

    def finish_apply(out):
        put(0, fields[0, 0], fields[0, 1])
        products((8,), True, out)

    row16 = lax.broadcasted_iota(jnp.int32, (2 * SUB, lanes), 0)
    lane16 = lax.broadcasted_iota(jnp.int32, (2 * SUB, lanes), 1)

    def start_reduce(j, values):
        table = jnp.zeros((2 * SUB, lanes), jnp.float32)
        for k, value in enumerate(values):
            table = jnp.where(row16 == k, jnp.sum(value, axis=0, keepdims=True), table)
        table = jnp.sum(table, axis=1, keepdims=True)
        row = jnp.sum(jnp.where(row16 == lane16, table, 0.0), axis=0, keepdims=True)
        row_one[j] = row
        for k in range(1, n_xy):
            cp = remote(row_one.at[j], red_one.at[j, me_xy], one_send.at[j, k], one_recv.at[j, me_xy],
                        {"xy": lax.rem(me_xy + k, n_xy)})
            cp.start()
            pending.append(cp)
        red_one[j, me_xy] = row

    def middle_reduce(j):
        for k in range(1, n_xy):
            p = lax.rem(me_xy + n_xy - k, n_xy)
            remote(row_one.at[j], red_one.at[j, p], one_send.at[j, k], one_recv.at[j, p], {"xy": p}).wait_recv()
        row = red_one[j, 0]
        for k in range(1, n_xy):
            row = row + red_one[j, k]
        row_two[j] = row
        for k in range(1, n_two):
            cp = remote(row_two.at[j], red_two.at[j, me_two], two_send.at[j, k], two_recv.at[j, me_two], two_peer(k)[1])
            cp.start()
            pending.append(cp)
        red_two[j, me_two] = row

    def end_reduce(j, count):
        for k in range(1, n_two):
            p, device = two_peer(n_two - k)
            remote(row_two.at[j], red_two.at[j, p], two_send.at[j, k], two_recv.at[j, p], device).wait_recv()
        row = red_two[j, 0]
        for k in range(1, n_two):
            row = row + red_two[j, k]
        return [jnp.broadcast_to(row[:, k:k + 1], (1, lanes)) for k in range(count)]

    def load(ref):
        return (ref[0], ref[1])

    def store(ref, value):
        ref[0] = value[0]
        ref[1] = value[1]

    def dots(vector_refs, q):
        values = []
        for ref in vector_refs:
            values.extend(cmul_conj(load(ref), q))
        values.append(q[0] * q[0] + q[1] * q[1])
        return values

    waits = send_halo(0, src)
    for at, d in enumerate(ARRIVAL):
        if d == 6:
            set_y(src)
        elif d == 4:
            set_x(0, src, waits)
        elif d == 0:
            set_t(0, waits)
        elif d == 2:
            set_z(0, waits)
        loads[at].wait()
        convert(d)
        products((d,), at == 0, fields.at[0] if at == 7 else None)
    loads[8].wait()
    convert(8)
    raw = fields.at[1]
    finish_apply(raw)

    def apply(e, ref, out, j):
        set_y(ref)
        products((6, 7), True)
        middle_reduce(j)
        set_x(e, ref, waits)
        products((4, 5), False)
        set_t(e, waits)
        set_z(e, waits)
        products((0, 1, 2, 3), False, fields.at[0])
        finish_apply(out)

    source = load(src)
    q = load(raw)
    start_reduce(0, dots([src], q) + [source[0] * source[0] + source[1] * source[1]])
    waits = send_halo(1, raw)
    product = fields.at[2]
    apply(1, raw, product, 0)
    dot_re, dot_im, q_sq, norm_sq = end_reduce(0, 4)
    source_norm = jnp.sqrt(norm_sq)
    scale = 1.0 / source_norm
    store(vs.at[0], cscale(load(src), scale))
    store(qs.at[0], cscale(load(raw), scale))
    store(product, cscale(load(product), scale))
    g = [(dot_re * scale * scale, dot_im * scale * scale)]
    q_sq = q_sq * scale * scale

    columns = []
    low = [[None] * ITERS for _ in range(ITERS)]
    inv_diag, forward = [], []

    def factor_row(j):
        entries = []
        for k in range(j + 1):
            total = cmul_conj(columns[j][0], columns[k][0])
            for m in range(1, k + 2):
                term = cmul_conj(columns[j][m], columns[k][m])
                total = (total[0] + term[0], total[1] + term[1])
            entries.append(total)
        for k in range(j):
            total = entries[k]
            for m in range(k):
                total = csub(total, cmul_conj(low[k][m], low[j][m]))
            low[j][k] = cscale(total, inv_diag[k])
        diag = entries[j][0]
        for m in range(j):
            diag = diag - (low[j][m][0] * low[j][m][0] + low[j][m][1] * low[j][m][1])
        inv_diag.append(1.0 / jnp.sqrt(diag))
        total = (source_norm * columns[j][0][0], -source_norm * columns[j][0][1])
        for m in range(j):
            total = csub(total, cmul(low[j][m], forward[m]))
        forward.append(cscale(total, inv_diag[j]))

    zero = jnp.zeros((1, lanes), jnp.float32)
    for j in range(ITERS):
        length_sq = q_sq
        for re, im in g:
            length_sq = length_sq - (re * re + im * im)
        length = jnp.sqrt(length_sq)
        columns.append(g[:j] + [(g[j][0] + 1.0, g[j][1]), (length, zero)])
        if j < ITERS - 1:
            scale = 1.0 / length
            v = load(qs.at[j])
            q = load(product)
            for i in range(j + 1):
                v = csub(v, cmul(g[i], load(vs.at[i])))
                q = csub(q, cmul(g[i], load(qs.at[i])))
            store(qs.at[j + 1], cscale(q, scale))
            store(vs.at[j + 1], cscale(v, scale))
            last = j + 1 == ITERS - 1
            start_reduce(j + 1, dots([vs.at[i] for i in range(j + 2)], load(qs.at[j + 1])))
            if not last:
                waits = send_halo(j + 2, qs.at[j + 1])
            factor_row(j)
            if last:
                middle_reduce(j + 1)
            else:
                product = fields.at[j + 3]
                apply(j + 2, qs.at[j + 1], product, j + 1)
            got = end_reduce(j + 1, 2 * (j + 2) + 1)
            g = [(got[2 * i], got[2 * i + 1]) for i in range(j + 2)]
            q_sq = got[2 * (j + 2)]
        else:
            factor_row(j)

    coeffs = [None] * ITERS
    for j in reversed(range(ITERS)):
        total = forward[j]
        for m in range(j + 1, ITERS):
            total = csub(total, cmul_conj(low[m][j], coeffs[m]))
        coeffs[j] = cscale(total, inv_diag[j])

    answer = cmul(coeffs[0], load(vs.at[0]))
    left = csub(load(src), cmul(coeffs[0], load(qs.at[0])))
    for j in range(1, ITERS):
        term = cmul(coeffs[j], load(vs.at[j]))
        answer = (answer[0] + term[0], answer[1] + term[1])
        left = csub(left, cmul(coeffs[j], load(qs.at[j])))
    store(sol_ref, answer)
    store(res_ref, csub(left, answer))

    shape = hes_ref.shape[1:]
    part = lax.broadcasted_iota(jnp.int32, shape, 0)
    row = lax.broadcasted_iota(jnp.int32, shape, 1)
    for j in range(ITERS):
        table = jnp.zeros(shape, jnp.float32)
        for i in range(j + 2):
            re, im = (x[:, :shape[1]] for x in columns[j][i])
            table = jnp.where(row == i, jnp.where(part == 0, re, im), table)
        hes_ref[j] = table

    for cp in pending:
        cp.wait_send()


def hand_on(*refs):
    half = len(refs) // 2
    for i in range(half):
        refs[half + i][...] = refs[i][...]


def solution(mesh):
    sizes = tuple(mesh.shape[a] for a in ("ta", "gz", "xy"))

    def per_device(source, inverse, coarse_links):
        comp, lanes = source.shape[1], source.shape[4]
        f32 = jnp.float32
        field = (2, comp, lanes)
        mats = (9, comp, comp, lanes)
        n_two = sizes[0] * sizes[1]
        dma = pltpu.SemaphoreType.DMA
        hbm = pl.BlockSpec(memory_space=pl.ANY)
        vmem = pl.BlockSpec(memory_space=pltpu.VMEM)
        sol, res, hes = pl.pallas_call(
            functools.partial(kernel, sizes),
            out_shape=(
                jax.ShapeDtypeStruct(field, f32),
                jax.ShapeDtypeStruct(field, f32),
                jax.ShapeDtypeStruct((ITERS, 2, ITERS + 1), f32),
            ),
            in_specs=[hbm, hbm, hbm],
            out_specs=(vmem, vmem, vmem),
            scratch_shapes=[
                pltpu.VMEM((9, 2, comp, comp, lanes), coarse_links.dtype),
                pltpu.VMEM(mats, f32),
                pltpu.VMEM(mats, f32),
                pltpu.VMEM(mats, f32),
                pltpu.VMEM((8, 3, comp, lanes), f32),
                pltpu.VMEM((3, comp, SUB, lanes), f32),
                pltpu.VMEM(field, f32),
                pltpu.VMEM((ITERS + 1, *field), f32),
                pltpu.VMEM((ITERS, *field), f32),
                pltpu.VMEM((ITERS, *field), f32),
                pltpu.VMEM((ITERS, 2, *field), f32),
                pltpu.VMEM((ITERS, 2, *field), f32),
                pltpu.VMEM((ITERS, 2, 2, SUB, lanes), f32),
                pltpu.VMEM((ITERS, 2, 2, SUB, lanes), f32),
                pltpu.VMEM((ITERS, sizes[2], 1, lanes), f32),
                pltpu.VMEM((ITERS, n_two, 1, lanes), f32),
                pltpu.VMEM((ITERS, 1, lanes), f32),
                pltpu.VMEM((ITERS, 1, lanes), f32),
                dma((9,)),
                dma,
                dma((ITERS, 2)), dma((ITERS, 2)),
                dma((ITERS, 2)), dma((ITERS, 2)),
                dma((ITERS, 2)), dma((ITERS, 2)),
                dma((ITERS, sizes[2])), dma((ITERS, sizes[2])),
                dma((ITERS, n_two)), dma((ITERS, n_two)),
            ],
            compiler_params=pltpu.CompilerParams(
                collective_id=0, has_side_effects=True, vmem_limit_bytes=60 * 1024 * 1024),
        )(
            source.reshape(field),
            inverse.reshape(2, comp, comp, lanes),
            coarse_links.reshape(8, 2, comp, comp, lanes),
        )
        results = (sol, res, hes)
        sol, res, hes = pl.pallas_call(
            hand_on,
            out_shape=tuple(jax.ShapeDtypeStruct(x.shape, x.dtype) for x in results),
            in_specs=[vmem] * 3,
            out_specs=(vmem,) * 3,
        )(*results)
        return sol.reshape(source.shape), res.reshape(source.shape), hes.transpose(1, 2, 0)

    specs = (
        P(None, None, "ta", "gz", "xy"),
        P(None, None, None, "ta", "gz", "xy"),
        P(None, None, None, None, "ta", "gz", "xy"),
    )
    return jax.shard_map(
        per_device,
        mesh=mesh,
        in_specs=specs,
        out_specs=(specs[0], specs[0], P()),
        check_vma=False,
    )
```
